512 devices in a mesh: gx: 4 (over y_hi, core), gy: 16 (over z), gz: 8 (over y_lo, x).
Axes of the slice: x: 4, y: 4 (y_hi: 2, y_lo: 2; y = y_hi * 2 + y_lo), z: 16, core: 2. Of those that a mesh axis runs over, the one named last changes fastest.
Arguments:
- heat_level_grid: float32 [256, 1024, 512], P('gz', 'gy', 'gx'), may hold values from -16 to 16, as said below
- interval_first_class: int32 [1], replicated, may hold values from 0 to 95
- interval_beyond_class: int32 [1], replicated, may hold values from 128 to 256
Outputs:
- magnitude: float32 [256, 1024, 512], P('gz', 'gy', 'gx')
- histogram: float32 [256], replicated
- stats: float32 [4], replicated
The draws below stay inside these ranges and needn't reach their ends.
Inputs may be any that keep to these rules, and one draw needn't show every extreme that they name: `heat_level_grid`: each entry is a rough value times an amplitude that is constant on blocks of 8 x 4 x 4 cells (z, y, x) and varies over a factor of 16 between blocks.
All inputs are finite; a program needn't handle non-finite values.
Results may differ from the reference program's by a relative error of at most 0.0003.
Values sent between devices are 32-bit elements; how exact they have to be, the bound alone decides.
No kernel may reach another device: no remote copies, remote signals or barrier semaphores. Data moves between devices by JAX's collectives and lax.ppermute only.
A program may use at most 64 MiB of HBM per device.

```python
import math
import jax
import jax.numpy as jnp

BINS = 256
NX = 512
NY = 1024
NZ = 256


def draw_heat_level_grid(key, part):
    first_key, second_key = jax.random.split(jax.random.fold_in(key, 11))
    coarse = jax.random.uniform(first_key, (NZ // 8, NY // 4, NX // 4), jnp.float32, math.log(0.25), math.log(4.0))
    amplitude = jnp.exp(coarse)
    amplitude = jnp.repeat(jnp.repeat(jnp.repeat(amplitude, 8, axis=0), 4, axis=1), 4, axis=2)
    noise = jnp.clip(jax.random.normal(second_key, (NZ, NY, NX), jnp.float32), -4.0, 4.0)
    return (amplitude * noise).astype(jnp.float32)


def setup_inputs(seed: int = 0) -> dict:
    key_list = jax.random.split(jax.random.key(seed), 4)
    return {
        "heat_level_grid": draw_heat_level_grid(jax.random.fold_in(key_list[3], 71), 0),
        "interval_first_class": jax.random.randint(key_list[1], (1,), 0, 96).astype(jnp.int32),
        "interval_beyond_class": jax.random.randint(key_list[2], (1,), 128, BINS + 1).astype(jnp.int32),
    }


stencil_coefficients = (0.8, -0.2, 4.0 / 105.0, -1.0 / 280.0)
grad_range = 12.0

def directional_rate(field, direction_length_count):
    running = jnp.zeros_like(field)
    for offset, coefficient in enumerate(stencil_coefficients, start=1):
        running = running + coefficient * (jnp.roll(field, -offset, direction_length_count) - jnp.roll(field, offset, direction_length_count))
    return running

def reference(heat_level_grid, interval_first_class, interval_beyond_class):
    slope_norm_square = jnp.zeros_like(heat_level_grid)
    for direction_length_count in range(3):
        slope_in_direction = directional_rate(heat_level_grid, direction_length_count)
        slope_norm_square = slope_norm_square + slope_in_direction * slope_in_direction
    magnitude = jnp.sqrt(slope_norm_square + 1.0) - 1.0
    position = jnp.clip(magnitude * (BINS / grad_range), 0.5, BINS - 0.5)
    low_bin = jnp.minimum(jnp.floor(position - 0.5), BINS - 2).astype(jnp.int32)
    fraction = position - 0.5 - low_bin.astype(position.dtype)
    flat_low = low_bin.ravel()
    flat_frac = fraction.ravel()
    counts = jax.ops.segment_sum(1.0 - flat_frac, flat_low, BINS) + jax.ops.segment_sum(flat_frac, flat_low + 1, BINS)
    total_cells = NX * NY * NZ
    histogram = counts * (BINS / total_cells)
    lower_edge = interval_first_class[0]
    upper_edge = interval_beyond_class[0]
    high_bin = low_bin + 1
    inside_low = (low_bin >= lower_edge) & (low_bin < upper_edge)
    inside_high = (high_bin >= lower_edge) & (high_bin < upper_edge)
    weight = jnp.where(inside_low, 1.0 - fraction, 0.0) + jnp.where(inside_high, fraction, 0.0)
    lowest = jnp.min(magnitude + grad_range * (1.0 - weight))
    highest = jnp.max(weight * magnitude)
    weighted_sum = jnp.sum(weight * magnitude) / total_cells
    weighted_count = jnp.sum(weight) / total_cells
    stats = jnp.stack([lowest, highest, weighted_sum, weighted_count])
    return (magnitude, histogram, stats)
```

```python
import jax
import jax.numpy as jnp
import numpy as np
from jax import lax
from jax.experimental import pallas as pl
from jax.experimental.pallas import tpu as pltpu
from jax.sharding import Mesh
from jax.sharding import PartitionSpec as P

BINS = 256
GX = ("gx_0", "gx_1")
GZ = ("gz_0", "gz_1")
GX_GZ = ("gx_0", "gx_1", "gz_0", "gz_1")
COEF = tuple(float(np.float32(c)) for c in (0.8, -0.2, 4.0 / 105.0, -1.0 / 280.0))
GRAD_RANGE = 12.0
NZ, NY, NX = 32, 64, 128
STRIDE = NY + 16
ROUNDER = 49152.0


def split3(a):
    high = a.astype(jnp.bfloat16)
    rest = a - high.astype(jnp.float32)
    mid = rest.astype(jnp.bfloat16)
    low = (rest - mid.astype(jnp.float32)).astype(jnp.bfloat16)
    return high, mid, low


def correction_matrix():
    table = np.zeros((8, NX), np.float32)
    for j in range(4):
        for k in range(1, 5):
            i = NX + j - k
            if i < NX:
                table[j, i] = COEF[k - 1]
            i = k - 4 + j
            if i >= 0:
                table[4 + j, i] = -COEF[k - 1]
    high = table.astype(jnp.bfloat16)
    rest = table - high.astype(np.float32)
    mid = rest.astype(jnp.bfloat16)
    low = (rest - mid.astype(np.float32)).astype(jnp.bfloat16)
    return np.concatenate([high, mid, high, low, mid, high], axis=0)


def pack_kernel(x_ref, xlo_ref, xhi_ref, ylo_ref, yhi_ref, zlo_ref, zhi_ref):
    for i in range(NZ * NY // 128):
        block = x_ref[2 * i : 2 * i + 2].reshape(128, NX)
        turned = block.T
        xlo_ref[:, i * 128 : (i + 1) * 128] = turned[0:4]
        xhi_ref[:, i * 128 : (i + 1) * 128] = turned[NX - 4 :]
    ylo_ref[...] = x_ref[:, 0:4, :]
    yhi_ref[...] = x_ref[:, NY - 4 :, :]
    zlo_ref[...] = x_ref[0:4]
    zhi_ref[...] = x_ref[NZ - 4 :]


def pack(x):
    f32 = jnp.float32
    return pl.pallas_call(
        pack_kernel,
        out_shape=(
            jax.ShapeDtypeStruct((4, NZ * NY), f32),
            jax.ShapeDtypeStruct((4, NZ * NY), f32),
            jax.ShapeDtypeStruct((NZ, 4, NX), f32),
            jax.ShapeDtypeStruct((NZ, 4, NX), f32),
            jax.ShapeDtypeStruct((4, NY, NX), f32),
            jax.ShapeDtypeStruct((4, NY, NX), f32),
        ),
        name="pack",
    )(x)


def main_kernel(
    first_ref, beyond_ref, c_ref, xlo_ref, xhi_ref, xleft_ref, xright_ref,
    x_hbm, ybelow_hbm, yabove_hbm, zbelow_hbm, zabove_hbm,
    mag_ref, red_ref,
    ext_ref, corr_ref, cell_ref, acc_ref, stat_ref, sems,
):
    copies = [
        pltpu.make_async_copy(x_hbm, ext_ref.at[4 : 4 + NZ, 8 : 8 + NY], sems.at[0]),
        pltpu.make_async_copy(zbelow_hbm, ext_ref.at[0:4, 8 : 8 + NY], sems.at[1]),
        pltpu.make_async_copy(zabove_hbm, ext_ref.at[4 + NZ :, 8 : 8 + NY], sems.at[2]),
        pltpu.make_async_copy(ybelow_hbm, ext_ref.at[4 : 4 + NZ, 4:8], sems.at[3]),
        pltpu.make_async_copy(yabove_hbm, ext_ref.at[4 : 4 + NZ, 8 + NY : 12 + NY], sems.at[4]),
    ]
    for copy in copies:
        copy.start()

    for i in range(NZ * NY // 128):
        cut = slice(i * 128, (i + 1) * 128)
        delta = jnp.concatenate(
            [xright_ref[:, cut] - xlo_ref[:, cut], xleft_ref[:, cut] - xhi_ref[:, cut]], axis=0
        )
        h, m, l = split3(delta)
        left = jnp.concatenate([h, h, m, h, m, l], axis=0)
        corr_ref[cut, :] = lax.dot_general(
            left, c_ref[...], (((0,), (0,)), ((), ())), preferred_element_type=jnp.float32
        )
    acc_ref[...] = jnp.zeros_like(acc_ref)
    stat_ref[0] = jnp.zeros((8, NX), jnp.float32)
    stat_ref[1] = jnp.full((8, NX), -3.0e38, jnp.float32)
    stat_ref[2] = jnp.full((8, NX), 3.0e38, jnp.float32)
    for copy in copies:
        copy.wait()

    first = first_ref[0].astype(jnp.float32)
    beyond = beyond_ref[0].astype(jnp.float32)
    rows_ref = ext_ref.reshape((NZ + 8) * STRIDE, NX)
    ids = lax.broadcasted_iota(jnp.int32, (16, NX), 0).astype(jnp.float32).astype(jnp.bfloat16)

    def cells(z, slot):
        base = (z + 4) * STRIDE + 8

        def at(offset):
            return rows_ref[pl.ds(base + offset, NY), :]

        center = at(0)
        gz = gy = gx = None
        for k in range(1, 5):
            c = COEF[k - 1]
            dz = c * (at(k * STRIDE) - at(-k * STRIDE))
            dy = c * (at(k) - at(-k))
            dx = c * (pltpu.roll(center, NX - k, 1) - pltpu.roll(center, k, 1))
            gz = dz if gz is None else gz + dz
            gy = dy if gy is None else gy + dy
            gx = dx if gx is None else gx + dx
        gx = gx + corr_ref[pl.ds(pl.multiple_of(z * NY, NY), NY), :]
        norm = gz * gz + gy * gy + gx * gx
        mag = jnp.sqrt(norm + 1.0) - 1.0
        mag_ref[z] = mag
        place = jnp.clip(mag * (BINS / GRAD_RANGE), 0.5, BINS - 0.5) - 0.5
        low = jnp.minimum(jnp.floor(place), BINS - 2.0)
        frac = place - low
        inside_low = (low >= first) & (low < beyond)
        inside_high = (low >= first - 1.0) & (low < beyond - 1.0)
        weight = jnp.where(inside_low, 1.0 - frac, 0.0) + jnp.where(inside_high, frac, 0.0)
        wm = weight * mag
        bottom = mag + GRAD_RANGE * (1.0 - weight)
        parts = lambda a: a.reshape(NY // 8, 8, NX)
        stat_ref[0] += jnp.sum(parts(wm), axis=0)
        stat_ref[1] = jnp.maximum(stat_ref[1], jnp.max(parts(wm), axis=0))
        stat_ref[2] = jnp.minimum(stat_ref[2], jnp.min(parts(bottom), axis=0))
        coarse = jnp.floor(low * 0.0625)
        frac_high = (frac + ROUNDER) - ROUNDER
        cell_ref[slot, 0] = coarse
        cell_ref[slot, 1] = low - 16.0 * coarse
        cell_ref[slot, 2] = frac_high
        cell_ref[slot, 3] = frac - frac_high

    def hist(slot):
        one = jnp.ones((16, NX), jnp.bfloat16)
        zero = jnp.zeros((16, NX), jnp.bfloat16)
        ones, highs, lows, fines = [], [], [], []
        for g in range(8):
            og, hg, lg, fg = [], [], [], []
            for j in range(8):
                r = g * 8 + j

                def row(q):
                    return jnp.broadcast_to(cell_ref[slot, q, r : r + 1, :], (16, NX)).astype(jnp.bfloat16)

                mask = row(0) == ids
                og.append(jnp.where(mask, one, zero))
                hg.append(jnp.where(mask, row(2), zero))
                lg.append(jnp.where(mask, row(3), zero))
                fg.append(jnp.where(row(1) == ids, one, zero))
            ones.append(jnp.concatenate(og, axis=1))
            highs.append(jnp.concatenate(hg, axis=1))
            lows.append(jnp.concatenate(lg, axis=1))
            fines.append(jnp.concatenate(fg, axis=1))
        left = jnp.concatenate(ones + highs + lows, axis=0)
        right = jnp.concatenate(fines, axis=0)
        acc_ref[...] += lax.dot_general(
            left, right, (((1,), (1,)), ((), ())), preferred_element_type=jnp.float32
        )

    cells(0, 0)

    def step(z, carry):
        hist((z - 1) % 2)
        cells(z, z % 2)
        return carry

    lax.fori_loop(1, NZ, step, 0)
    hist((NZ - 1) % 2)

    lane = lax.broadcasted_iota(jnp.int32, (16, NX), 1)
    sub = lax.broadcasted_iota(jnp.int32, (16, NX), 0)
    sums = []
    for w in range(3):
        total = jnp.zeros((16, NX), jnp.float32)
        for g in range(8):
            at_row = w * 128 + g * 16
            total = total + jnp.where(lane // 16 == g, acc_ref[at_row : at_row + 16, :], 0.0)
        for shift in (64, 32, 16):
            total = total + pltpu.roll(total, shift, 1)
        sums.append(total)
    upper = sums[1] + sums[2]
    beside = pltpu.roll(upper, 1, 1)
    carried = jnp.where(sub == 0, 0.0, pltpu.roll(beside, 1, 0))
    counts = sums[0] - upper + jnp.where(lane % 16 == 0, carried, beside)
    tops = [
        jnp.sum(jnp.where(sub == 8 * h + lane // 16, counts, 0.0), axis=0, keepdims=True)
        for h in range(2)
    ]
    tile = jnp.concatenate(
        tops
        + [
            jnp.sum(stat_ref[0], axis=0, keepdims=True),
            jnp.max(stat_ref[1], axis=0, keepdims=True),
            jnp.min(stat_ref[2], axis=0, keepdims=True),
            jnp.zeros((3, NX), jnp.float32),
        ],
        axis=0,
    )
    red_ref[...] = jnp.broadcast_to(tile[None], red_ref.shape)


def main(x, edges, halos, first, beyond, peers):
    xlo, xhi = edges
    xleft, xright, ybelow, yabove, zbelow, zabove = halos
    smem = pl.BlockSpec(memory_space=pltpu.SMEM)
    vmem = pl.BlockSpec(memory_space=pltpu.VMEM)
    anywhere = pl.BlockSpec(memory_space=pl.ANY)
    return pl.pallas_call(
        main_kernel,
        in_specs=[smem, smem] + [vmem] * 5 + [anywhere] * 5,
        out_specs=(vmem, vmem),
        out_shape=(
            jax.ShapeDtypeStruct((NZ, NY, NX), jnp.float32),
            jax.ShapeDtypeStruct((peers, 8, NX), jnp.float32),
        ),
        scratch_shapes=[
            pltpu.VMEM((NZ + 8, STRIDE, NX), jnp.float32),
            pltpu.VMEM((NZ * NY, NX), jnp.float32),
            pltpu.VMEM((2, 4, NY, NX), jnp.float32),
            pltpu.VMEM((384, NX), jnp.float32),
            pltpu.VMEM((3, 8, NX), jnp.float32),
            pltpu.SemaphoreType.DMA((5,)),
        ],
        name="cells",
    )(first, beyond, correction_matrix(), xlo, xhi, xleft, xright, x, ybelow, yabove, zbelow, zabove)


def merged(a):
    summed = jnp.sum(a[:, 0:3, :], axis=0)
    high = jnp.max(a[:, 3:4, :], axis=0)
    low = jnp.min(a[:, 4:5, :], axis=0)
    return summed, high, low


def merge_kernel(a_ref, out_ref):
    summed, high, low = merged(a_ref)
    tile = jnp.concatenate([summed, high, low, jnp.zeros((3, NX), jnp.float32)], axis=0)
    out_ref[...] = jnp.broadcast_to(tile[None], out_ref.shape)


def final_kernel(first_ref, beyond_ref, a_ref, hist_ref, stats_ref):
    summed, high, low = merged(a_ref)
    cells = 134217728.0
    counts = summed[0:2]
    hist_ref[...] = counts * (BINS / cells)
    bins = lax.broadcasted_iota(jnp.int32, (2, NX), 0) * NX + lax.broadcasted_iota(jnp.int32, (2, NX), 1)
    inside = (bins >= first_ref[0]) & (bins < beyond_ref[0])
    stats_ref[0] = jnp.min(low)
    stats_ref[1] = jnp.max(high)
    stats_ref[2] = jnp.sum(summed[2:3]) / cells
    stats_ref[3] = jnp.sum(jnp.where(inside, counts, 0.0)) / cells


def shifted(part, axis, step):
    count = lax.axis_size(axis)
    return lax.ppermute(part, axis, [(i, (i + step) % count) for i in range(count)])


def on_device(x, first, beyond):
    xlo, xhi, ylo, yhi, zlo, zhi = pack(x)
    halos = (
        shifted(xhi, GX, 1),
        shifted(xlo, GX, -1),
        shifted(yhi, "gy", 1),
        shifted(ylo, "gy", -1),
        shifted(zhi, GZ, 1),
        shifted(zlo, GZ, -1),
    )
    mag, red = main(x, (xlo, xhi), halos, first, beyond, lax.axis_size(GX_GZ))
    red = lax.all_to_all(red, GX_GZ, 0, 0)
    red = pl.pallas_call(
        merge_kernel,
        out_shape=jax.ShapeDtypeStruct((lax.axis_size("gy"), 8, NX), jnp.float32),
        name="merge",
    )(red)
    red = lax.all_to_all(red, "gy", 0, 0)
    smem = pl.BlockSpec(memory_space=pltpu.SMEM)
    vmem = pl.BlockSpec(memory_space=pltpu.VMEM)
    hist, stats = pl.pallas_call(
        final_kernel,
        in_specs=[smem, smem, vmem],
        out_specs=(vmem, smem),
        out_shape=(
            jax.ShapeDtypeStruct((2, NX), jnp.float32),
            jax.ShapeDtypeStruct((4,), jnp.float32),
        ),
        name="final",
    )(first, beyond, red)
    return mag, hist.reshape(BINS), stats


def solution(mesh):
    finer = Mesh(
        mesh.devices.reshape(2, 2, mesh.shape["gy"], 2, 4), ("gx_0", "gx_1", "gy", "gz_0", "gz_1")
    )
    return jax.shard_map(
        on_device,
        mesh=finer,
        in_specs=(P(GZ, "gy", GX), P(), P()),
        out_specs=(P(GZ, "gy", GX), P(), P()),
        check_vma=False,
    )
```

```python
import jax
import jax.numpy as jnp
import numpy as np
from jax import lax
from jax.experimental import pallas as pl
from jax.experimental.pallas import tpu as pltpu
from jax.sharding import Mesh
from jax.sharding import PartitionSpec as P


BINS = 256
GX = ("gx_0", "gx_1")
GZ = ("gz_0", "gz_1")
GX_GZ = ("gx_0", "gx_1", "gz_0", "gz_1")
COEF = tuple(float(np.float32(c)) for c in (0.8, -0.2, 4.0 / 105.0, -1.0 / 280.0))
GRAD_RANGE = 12.0
NZ, NY, NX = 32, 64, 128
ROW = NY + 16
ROUNDER = 49152.0


def split3(a):
    high = a.astype(jnp.bfloat16)
    rest = a - high.astype(jnp.float32)
    mid = rest.astype(jnp.bfloat16)
    low = (rest - mid.astype(jnp.float32)).astype(jnp.bfloat16)
    return high, mid, low


def correction_matrix():
    table = np.zeros((8, NX), np.float32)
    for j in range(4):
        for k in range(1, 5):
            i = NX + j - k
            if i < NX:
                table[j, i] = COEF[k - 1]
            i = k - 4 + j
            if i >= 0:
                table[4 + j, i] = -COEF[k - 1]
    high = table.astype(jnp.bfloat16)
    rest = table - high.astype(np.float32)
    mid = rest.astype(jnp.bfloat16)
    low = (rest - mid.astype(np.float32)).astype(jnp.bfloat16)
    return np.concatenate([high, mid, high, low, mid, high], axis=0)


def in_vmem(a):
    return pltpu.with_memory_space_constraint(a, pltpu.VMEM)


def vmem_out(*shape):
    return pltpu.VMEM(shape, jnp.float32)


VMEM = pl.BlockSpec(memory_space=pltpu.VMEM)
SMEM = pl.BlockSpec(memory_space=pltpu.SMEM)


def pack_kernel(x_ref, copy_ref, xlo_ref, xhi_ref, ylo_ref, yhi_ref, zlo_ref, zhi_ref):
    for i in range(NZ * NY // 128):
        block = x_ref[2 * i : 2 * i + 2].reshape(128, NX)
        turned = block.T
        xlo_ref[:, i * 128 : (i + 1) * 128] = turned[0:4]
        xhi_ref[:, i * 128 : (i + 1) * 128] = turned[NX - 4 :]
    ylo_ref[...] = x_ref[:, 0:4, :]
    yhi_ref[...] = x_ref[:, NY - 4 :, :]
    zlo_ref[...] = x_ref[0:4]
    zhi_ref[...] = x_ref[NZ - 4 :]
    copy_ref[...] = x_ref[...]


def pack(x):
    return pl.pallas_call(
        pack_kernel,
        in_specs=[VMEM],
        out_specs=(VMEM,) * 7,
        out_shape=(
            vmem_out(NZ, NY, NX),
            vmem_out(4, NZ * NY),
            vmem_out(4, NZ * NY),
            vmem_out(NZ, 4, NX),
            vmem_out(NZ, 4, NX),
            vmem_out(4, NY, NX),
            vmem_out(4, NY, NX),
        ),
        name="pack",
    )(x)


def stencil(pairs):
    total = None
    for c, (after, before) in zip(COEF, pairs):
        term = c * (after - before)
        total = term if total is None else total + term
    return total


def xz_kernel(c_ref, x_ref, xlo_ref, xhi_ref, xleft_ref, xright_ref, zbelow_ref, zabove_ref, out_ref, corr_ref):
    for i in range(NZ * NY // 128):
        cut = slice(i * 128, (i + 1) * 128)
        delta = jnp.concatenate(
            [xright_ref[:, cut] - xlo_ref[:, cut], xleft_ref[:, cut] - xhi_ref[:, cut]], axis=0
        )
        h, m, l = split3(delta)
        left = jnp.concatenate([h, h, m, h, m, l], axis=0)
        corr_ref[2 * i : 2 * i + 2] = lax.dot_general(
            left, c_ref[...], (((0,), (0,)), ((), ())), preferred_element_type=jnp.float32
        ).reshape(2, NY, NX)

    def plane(z, fetch):
        center = x_ref[z]
        gx = stencil(
            [(pltpu.roll(center, NX - k, 1), pltpu.roll(center, k, 1)) for k in range(1, 5)]
        )
        gx = gx + corr_ref[z]
        gz = stencil([(fetch(k), fetch(-k)) for k in range(1, 5)])
        out_ref[z] = gx * gx + gz * gz

    for z in (0, 1, 2, 3, NZ - 4, NZ - 3, NZ - 2, NZ - 1):

        def fetch(k):
            at = z + k
            if at < 0:
                return zbelow_ref[at + 4]
            if at >= NZ:
                return zabove_ref[at - NZ]
            return x_ref[at]

        plane(z, fetch)

    def step(z, carry):
        plane(z, lambda k: x_ref[z + k])
        return carry

    lax.fori_loop(4, NZ - 4, step, 0, unroll=4)


def xz_squares(x, edges, halos):
    args = [correction_matrix()] + [in_vmem(a) for a in (x, *edges, *halos)]
    return pl.pallas_call(
        xz_kernel,
        in_specs=[VMEM] * 8,
        out_specs=VMEM,
        out_shape=vmem_out(NZ, NY, NX),
        scratch_shapes=[pltpu.VMEM((NZ, NY, NX), jnp.float32)],
        name="xz",
    )(*args)


def cells_kernel(
    first_ref, beyond_ref, x_ref, square_ref, ybelow_ref, yabove_ref,
    mag_ref, red_ref,
    rows_ref, cell0_ref, cell1_ref, stat_ref,
):
    pl.run_scoped(
        lambda *accs: cells_body(
            first_ref, beyond_ref, x_ref, square_ref, ybelow_ref, yabove_ref,
            mag_ref, red_ref,
            rows_ref, cell0_ref, cell1_ref, stat_ref, *accs,
        ),
        pltpu.ACC(mxu_id=0)((256, 256), jnp.float32),
        pltpu.ACC(mxu_id=1)((256, 256), jnp.float32),
    )


def cells_body(
    first_ref, beyond_ref, x_ref, square_ref, ybelow_ref, yabove_ref,
    mag_ref, red_ref,
    rows_ref, cell0_ref, cell1_ref, stat_ref, acc0_ref, acc1_ref,
):
    cell_refs = (cell0_ref, cell1_ref)
    acc_refs = (acc0_ref, acc1_ref)
    stat_ref[0] = jnp.zeros((8, NX), jnp.float32)
    stat_ref[1] = jnp.full((8, NX), -3.0e38, jnp.float32)
    stat_ref[2] = jnp.full((8, NX), 3.0e38, jnp.float32)
    before = first_ref[0].astype(jnp.float32) - 1.0
    beyond = beyond_ref[0].astype(jnp.float32)
    ids = lax.broadcasted_iota(jnp.int32, (16, NX), 0).astype(jnp.float32).astype(jnp.bfloat16)
    one = jnp.ones((16, NX), jnp.bfloat16)
    zero = jnp.zeros((16, NX), jnp.bfloat16)

    def cells(z, slot):
        cell_ref = cell_refs[slot]
        base = (z % 2) * ROW
        rows_ref[pl.ds(pl.multiple_of(base + 8, 8), NY), :] = x_ref[z]
        rows_ref[pl.ds(base + 4, 4), :] = ybelow_ref[z]
        rows_ref[pl.ds(base + 8 + NY, 4), :] = yabove_ref[z]

        def at(offset):
            return rows_ref[pl.ds(base + 8 + offset, NY), :]

        gy = stencil([(at(k), at(-k)) for k in range(1, 5)])
        norm = square_ref[z] + gy * gy + 1.0
        mag = norm * lax.rsqrt(norm) - 1.0
        mag_ref[z] = mag
        place = jnp.clip(mag * (BINS / GRAD_RANGE), 0.5, BINS - 0.5) - 0.5
        low = jnp.minimum(jnp.floor(place), BINS - 2.0)
        frac = place - low
        weight = jnp.clip(jnp.minimum(place - before, beyond - place), 0.0, 1.0)
        parts = lambda a: a.reshape(NY // 8, 8, NX)
        stat_ref[0] += jnp.sum(parts(weight * mag), axis=0)
        stat_ref[1] = jnp.maximum(stat_ref[1], jnp.max(parts(weight * mag), axis=0))
        stat_ref[2] = jnp.minimum(
            stat_ref[2], jnp.min(parts(mag + GRAD_RANGE * (1.0 - weight)), axis=0)
        )
        coarse = jnp.floor(low * 0.0625)
        frac_high = (frac + ROUNDER) - ROUNDER
        cell_ref[0] = coarse
        cell_ref[1] = low - 16.0 * coarse
        cell_ref[2] = frac_high
        cell_ref[3] = frac - frac_high

    def hist(slot):
        cell_ref = cell_refs[slot]

        def row(q, r):
            return jnp.broadcast_to(cell_ref[q, r : r + 1, :], (16, NX)).astype(jnp.bfloat16)

        for q in range(4):
            left, right = [], []
            for g in range(8):
                sides = []
                for r in (16 * q + 2 * g, 16 * q + 2 * g + 1):
                    coarse = row(0, r) == ids
                    finer = row(1, r) == ids
                    sides.append(
                        (
                            jnp.where(coarse, one, zero),
                            jnp.where(coarse, row(2, r), zero),
                            jnp.where(finer, one, zero),
                            jnp.where(finer, row(3, r), zero),
                        )
                    )
                joined = [jnp.concatenate(pair, axis=1) for pair in zip(*sides)]
                left += joined[:2]
                right += joined[2:]
            mxu = q % 2
            pltpu.matmul_push_rhs(jnp.concatenate(right, axis=0), q // 2, mxu, transpose=True)
            pltpu.matmul_acc_lhs(acc_refs[mxu], jnp.concatenate(left, axis=0), load_staged_rhs=q // 2)

    cells(0, 0)

    def step(i, carry):
        hist(0)
        cells(2 * i + 1, 1)
        hist(1)
        cells(2 * i + 2, 0)
        return carry

    lax.fori_loop(0, NZ // 2 - 1, step, 0)
    hist(0)
    cells(NZ - 1, 1)
    hist(1)

    both = pltpu.matmul_pop(acc0_ref) + pltpu.matmul_pop(acc1_ref)
    lane = lax.broadcasted_iota(jnp.int32, (32, NX), 1)
    total = jnp.zeros((32, NX), jnp.float32)
    for g in range(8):
        part = both[g * 32 : (g + 1) * 32, (g // 4) * NX : (g // 4 + 1) * NX]
        total = total + jnp.where(lane // 32 == g % 4, part, 0.0)
    for shift in (64, 32):
        total = total + pltpu.roll(total, shift, 1)
    lane = lax.broadcasted_iota(jnp.int32, (16, NX), 1)
    sub = lax.broadcasted_iota(jnp.int32, (16, NX), 0)
    plain = total[0:16]
    upper = total[16:32] + pltpu.roll(plain, NX - 16, 1)

    def repeated(a):
        a = jnp.where(lane % 32 < 16, a, 0.0)
        return a + pltpu.roll(a, 16, 1)

    plain = repeated(plain)
    upper = repeated(upper)
    beside = pltpu.roll(upper, 1, 1)
    carried = jnp.where(sub == 0, 0.0, pltpu.roll(beside, 1, 0))
    counts = plain - upper + jnp.where(lane % 16 == 0, carried, beside)
    tops = [
        jnp.sum(jnp.where(sub == 8 * h + lane // 16, counts, 0.0), axis=0, keepdims=True)
        for h in range(2)
    ]
    tile = jnp.concatenate(
        tops
        + [
            jnp.sum(stat_ref[0], axis=0, keepdims=True),
            jnp.max(stat_ref[1], axis=0, keepdims=True),
            jnp.min(stat_ref[2], axis=0, keepdims=True),
            jnp.zeros((3, NX), jnp.float32),
        ],
        axis=0,
    )
    red_ref[...] = jnp.broadcast_to(tile[None], red_ref.shape)


def cells(x, squares, halos, first, beyond, peers):
    args = [in_vmem(a) for a in (x, squares, *halos)]
    return pl.pallas_call(
        cells_kernel,
        in_specs=[SMEM, SMEM] + [VMEM] * 4,
        out_specs=(VMEM, VMEM),
        out_shape=(vmem_out(NZ, NY, NX), vmem_out(peers, 8, NX)),
        scratch_shapes=[
            pltpu.VMEM((2 * ROW, NX), jnp.float32),
            pltpu.VMEM((4, NY, NX), jnp.float32),
            pltpu.VMEM((4, NY, NX), jnp.float32),
            pltpu.VMEM((3, 8, NX), jnp.float32),
        ],
        input_output_aliases={3: 0},
        name="cells",
    )(first, beyond, *args)


def merged(a):
    summed = jnp.sum(a[:, 0:3, :], axis=0)
    high = jnp.max(a[:, 3:4, :], axis=0)
    low = jnp.min(a[:, 4:5, :], axis=0)
    return summed, high, low


def merge_kernel(a_ref, out_ref):
    summed, high, low = merged(a_ref)
    tile = jnp.concatenate([summed, high, low, jnp.zeros((3, NX), jnp.float32)], axis=0)
    out_ref[...] = jnp.broadcast_to(tile[None], out_ref.shape)


def merge(a, peers):
    return pl.pallas_call(
        merge_kernel,
        in_specs=[VMEM],
        out_specs=VMEM,
        out_shape=vmem_out(peers, 8, NX),
        name="merge",
    )(in_vmem(a))


def final_kernel(first_ref, beyond_ref, a_ref, hist_ref, stats_ref):
    summed, high, low = merged(a_ref)
    total_cells = 134217728.0
    counts = summed[0:2]
    hist_ref[...] = counts * (BINS / total_cells)
    bins = lax.broadcasted_iota(jnp.int32, (2, NX), 0) * NX + lax.broadcasted_iota(jnp.int32, (2, NX), 1)
    inside = (bins >= first_ref[0]) & (bins < beyond_ref[0])
    stats_ref[0] = jnp.min(low)
    stats_ref[1] = jnp.max(high)
    stats_ref[2] = jnp.sum(summed[2:3]) / total_cells
    stats_ref[3] = jnp.sum(jnp.where(inside, counts, 0.0)) / total_cells


def final(a, first, beyond):
    hist, stats = pl.pallas_call(
        final_kernel,
        in_specs=[SMEM, SMEM, VMEM],
        out_specs=(VMEM, SMEM),
        out_shape=(
            jax.ShapeDtypeStruct((2, NX), jnp.float32),
            jax.ShapeDtypeStruct((4,), jnp.float32),
        ),
        name="final",
    )(first, beyond, in_vmem(a))
    return hist.reshape(BINS), stats


def shifted(part, axis, step):
    count = lax.axis_size(axis)
    return lax.ppermute(part, axis, [(i, (i + step) % count) for i in range(count)])


def on_device(x, first, beyond):
    x, xlo, xhi, ylo, yhi, zlo, zhi = pack(x)
    xleft = shifted(xhi, GX, 1)
    xright = shifted(xlo, GX, -1)
    zbelow = shifted(zhi, GZ, 1)
    zabove = shifted(zlo, GZ, -1)
    ybelow = shifted(yhi, "gy", 1)
    yabove = shifted(ylo, "gy", -1)
    squares = xz_squares(x, (xlo, xhi), (xleft, xright, zbelow, zabove))
    mag, red = cells(x, squares, (ybelow, yabove), first, beyond, lax.axis_size(GX_GZ))
    red = lax.all_to_all(red, GX_GZ, 0, 0)
    red = merge(red, lax.axis_size("gy"))
    red = lax.all_to_all(red, "gy", 0, 0)
    hist, stats = final(red, first, beyond)
    return mag, hist, stats


def solution(mesh):
    finer = Mesh(
        mesh.devices.reshape(2, 2, mesh.shape["gy"], 2, 4), ("gx_0", "gx_1", "gy", "gz_0", "gz_1")
    )
    return jax.shard_map(
        on_device,
        mesh=finer,
        in_specs=(P(GZ, "gy", GX), P(), P()),
        out_specs=(P(GZ, "gy", GX), P(), P()),
        check_vma=False,
    )
```

```python
import jax
import jax.numpy as jnp
import numpy as np
from jax import lax
from jax.experimental import pallas as pl
from jax.experimental.pallas import tpu as pltpu
from jax.sharding import Mesh
from jax.sharding import PartitionSpec as P


BINS = 256
GX = ("gx_0", "gx_1")
GZ = ("gz_0", "gz_1")
GX_GZ = ("gx_0", "gx_1", "gz_0", "gz_1")
COEF = tuple(float(np.float32(c)) for c in (0.8, -0.2, 4.0 / 105.0, -1.0 / 280.0))
GRAD_RANGE = 12.0
NZ, NY, NX = 32, 64, 128
ROW = NY + 16
ROUNDER = 49152.0


def split3(a):
    high = a.astype(jnp.bfloat16)
    rest = a - high.astype(jnp.float32)
    mid = rest.astype(jnp.bfloat16)
    low = (rest - mid.astype(jnp.float32)).astype(jnp.bfloat16)
    return high, mid, low


def correction_matrix():
    table = np.zeros((8, NX), np.float32)
    for j in range(4):
        for k in range(1, 5):
            i = NX + j - k
            if i < NX:
                table[j, i] = COEF[k - 1]
            i = k - 4 + j
            if i >= 0:
                table[4 + j, i] = -COEF[k - 1]
    high = table.astype(jnp.bfloat16)
    rest = table - high.astype(np.float32)
    mid = rest.astype(jnp.bfloat16)
    low = (rest - mid.astype(np.float32)).astype(jnp.bfloat16)
    return np.concatenate([high, mid, high, low, mid, high], axis=0)


def in_vmem(a):
    return pltpu.with_memory_space_constraint(a, pltpu.VMEM)


def vmem_out(*shape):
    return pltpu.VMEM(shape, jnp.float32)


VMEM = pl.BlockSpec(memory_space=pltpu.VMEM)
SMEM = pl.BlockSpec(memory_space=pltpu.SMEM)


def odd(axis):
    return lax.axis_index(axis) % 2 == 1


def pack_kernel(x_hbm, x_ref, xa_ref, xb_ref, ya_ref, yb_ref, za_ref, zb_ref, sems):
    count = 4
    planes = NZ // count
    copies = [
        pltpu.make_async_copy(
            x_hbm.at[i * planes : (i + 1) * planes], x_ref.at[i * planes : (i + 1) * planes], sems.at[i]
        )
        for i in range(count)
    ]
    for copy in copies:
        copy.start()
    odd_x, odd_y, odd_z = odd(GX), odd("gy"), odd(GZ)
    for i in range(count):
        copies[i].wait()
        for j in range(i * planes // 2, (i + 1) * planes // 2):
            turned = x_ref[2 * j : 2 * j + 2].reshape(128, NX).T
            low, high = turned[0:4], turned[NX - 4 :]
            xa_ref[:, j * 128 : (j + 1) * 128] = jnp.where(odd_x, low, high)
            xb_ref[:, j * 128 : (j + 1) * 128] = jnp.where(odd_x, high, low)
        for z in range(i * planes, (i + 1) * planes):
            low, high = x_ref[z, 0:4], x_ref[z, NY - 4 :]
            ya_ref[z] = jnp.where(odd_y, low, high)
            yb_ref[z] = jnp.where(odd_y, high, low)
    low, high = x_ref[0:4], x_ref[NZ - 4 :]
    za_ref[...] = jnp.where(odd_z, low, high)
    zb_ref[...] = jnp.where(odd_z, high, low)


def pack(x):
    return pl.pallas_call(
        pack_kernel,
        in_specs=[pl.BlockSpec(memory_space=pl.ANY)],
        out_specs=(VMEM,) * 7,
        out_shape=(
            vmem_out(NZ, NY, NX),
            vmem_out(4, NZ * NY),
            vmem_out(4, NZ * NY),
            vmem_out(NZ, 4, NX),
            vmem_out(NZ, 4, NX),
            vmem_out(4, NY, NX),
            vmem_out(4, NY, NX),
        ),
        scratch_shapes=[pltpu.SemaphoreType.DMA((4,))],
        name="pack",
    )(x)


def stencil(pairs):
    total = None
    for c, (after, before) in zip(COEF, pairs):
        term = c * (after - before)
        total = term if total is None else total + term
    return total


def xz_kernel(c_ref, x_ref, xa_ref, xb_ref, from_xa_ref, from_xb_ref, from_za_ref, from_zb_ref, out_ref, corr_ref):
    odd_x, odd_z = odd(GX), odd(GZ)

    for i in range(NZ * NY // 128):
        cut = slice(i * 128, (i + 1) * 128)
        by_a = from_xa_ref[:, cut] - xb_ref[:, cut]
        by_b = from_xb_ref[:, cut] - xa_ref[:, cut]
        delta = jnp.concatenate(
            [jnp.where(odd_x, by_b, by_a), jnp.where(odd_x, by_a, by_b)], axis=0
        )
        h, m, l = split3(delta)
        left = jnp.concatenate([h, h, m, h, m, l], axis=0)
        corr_ref[2 * i : 2 * i + 2] = lax.dot_general(
            left, c_ref[...], (((0,), (0,)), ((), ())), preferred_element_type=jnp.float32
        ).reshape(2, NY, NX)

    def plane(z, fetch):
        center = x_ref[z]
        gx = stencil(
            [(pltpu.roll(center, NX - k, 1), pltpu.roll(center, k, 1)) for k in range(1, 5)]
        )
        gx = gx + corr_ref[z]
        gz = stencil([(fetch(k), fetch(-k)) for k in range(1, 5)])
        out_ref[z] = gx * gx + gz * gz

    for z in (0, 1, 2, 3, NZ - 4, NZ - 3, NZ - 2, NZ - 1):

        def fetch(k):
            at = z + k
            if at < 0:
                return jnp.where(odd_z, from_za_ref[at + 4], from_zb_ref[at + 4])
            if at >= NZ:
                return jnp.where(odd_z, from_zb_ref[at - NZ], from_za_ref[at - NZ])
            return x_ref[at]

        plane(z, fetch)

    def step(z, carry):
        plane(z, lambda k: x_ref[z + k])
        return carry

    lax.fori_loop(4, NZ - 4, step, 0, unroll=4)


def xz_squares(x, edges, halos):
    args = [correction_matrix()] + [in_vmem(a) for a in (x, *edges, *halos)]
    return pl.pallas_call(
        xz_kernel,
        in_specs=[VMEM] * 8,
        out_specs=VMEM,
        out_shape=vmem_out(NZ, NY, NX),
        scratch_shapes=[pltpu.VMEM((NZ, NY, NX), jnp.float32)],
        name="xz",
    )(*args)


def cells_kernel(
    first_ref, beyond_ref, x_ref, square_ref, from_ya_ref, from_yb_ref,
    mag_ref, mag_hbm, red_ref,
    rows_ref, cell0_ref, cell1_ref, stat_ref, sems,
):
    pl.run_scoped(
        lambda *accs: cells_body(
            first_ref, beyond_ref, x_ref, square_ref, from_ya_ref, from_yb_ref,
            mag_ref, mag_hbm, red_ref,
            rows_ref, cell0_ref, cell1_ref, stat_ref, sems, *accs,
        ),
        pltpu.ACC(mxu_id=0)((256, 256), jnp.float32),
        pltpu.ACC(mxu_id=1)((256, 256), jnp.float32),
    )


def cells_body(
    first_ref, beyond_ref, x_ref, square_ref, from_ya_ref, from_yb_ref,
    mag_ref, mag_hbm, red_ref,
    rows_ref, cell0_ref, cell1_ref, stat_ref, sems, acc0_ref, acc1_ref,
):
    cell_refs = (cell0_ref, cell1_ref)
    acc_refs = (acc0_ref, acc1_ref)
    stat_ref[0] = jnp.zeros((8, NX), jnp.float32)
    stat_ref[1] = jnp.full((8, NX), -3.0e38, jnp.float32)
    stat_ref[2] = jnp.full((8, NX), 3.0e38, jnp.float32)
    before = first_ref[0].astype(jnp.float32) - 1.0
    beyond = beyond_ref[0].astype(jnp.float32)
    odd_y = odd("gy")
    ids = lax.broadcasted_iota(jnp.int32, (16, NX), 0).astype(jnp.float32).astype(jnp.bfloat16)
    one = jnp.ones((16, NX), jnp.bfloat16)
    zero = jnp.zeros((16, NX), jnp.bfloat16)

    def cells(z, slot):
        cell_ref = cell_refs[slot]
        base = (z % 2) * ROW
        rows_ref[pl.ds(pl.multiple_of(base + 8, 8), NY), :] = x_ref[z]
        by_a, by_b = from_ya_ref[z], from_yb_ref[z]
        rows_ref[pl.ds(base + 4, 4), :] = jnp.where(odd_y, by_a, by_b)
        rows_ref[pl.ds(base + 8 + NY, 4), :] = jnp.where(odd_y, by_b, by_a)

        def at(offset):
            return rows_ref[pl.ds(base + 8 + offset, NY), :]

        gy = stencil([(at(k), at(-k)) for k in range(1, 5)])
        norm = square_ref[z] + gy * gy + 1.0
        mag = norm * lax.rsqrt(norm) - 1.0
        mag_ref[z] = mag
        place = jnp.clip(mag * (BINS / GRAD_RANGE), 0.5, BINS - 0.5) - 0.5
        low = jnp.minimum(jnp.floor(place), BINS - 2.0)
        frac = place - low
        weight = jnp.clip(jnp.minimum(place - before, beyond - place), 0.0, 1.0)
        parts = lambda a: a.reshape(NY // 8, 8, NX)
        stat_ref[0] += jnp.sum(parts(weight * mag), axis=0)
        stat_ref[1] = jnp.maximum(stat_ref[1], jnp.max(parts(weight * mag), axis=0))
        stat_ref[2] = jnp.minimum(
            stat_ref[2], jnp.min(parts(mag + GRAD_RANGE * (1.0 - weight)), axis=0)
        )
        coarse = jnp.floor(low * 0.0625)
        frac_high = (frac + ROUNDER) - ROUNDER
        cell_ref[0] = coarse
        cell_ref[1] = low - 16.0 * coarse
        cell_ref[2] = frac_high
        cell_ref[3] = frac - frac_high

    def hist(slot):
        cell_ref = cell_refs[slot]

        def row(q, r):
            return jnp.broadcast_to(cell_ref[q, r : r + 1, :], (16, NX)).astype(jnp.bfloat16)

        for q in range(4):
            left, right = [], []
            for g in range(8):
                sides = []
                for r in (16 * q + 2 * g, 16 * q + 2 * g + 1):
                    coarse = row(0, r) == ids
                    finer = row(1, r) == ids
                    sides.append(
                        (
                            jnp.where(coarse, one, zero),
                            jnp.where(coarse, row(2, r), zero),
                            jnp.where(finer, one, zero),
                            jnp.where(finer, row(3, r), zero),
                        )
                    )
                joined = [jnp.concatenate(pair, axis=1) for pair in zip(*sides)]
                left += joined[:2]
                right += joined[2:]
            mxu = q % 2
            pltpu.matmul_push_rhs(jnp.concatenate(right, axis=0), q // 2, mxu, transpose=True)
            pltpu.matmul_acc_lhs(acc_refs[mxu], jnp.concatenate(left, axis=0), load_staged_rhs=q // 2)

    def written(z, count):
        return pltpu.make_async_copy(mag_ref.at[pl.ds(z, count)], mag_hbm.at[pl.ds(z, count)], sems.at[0])

    cells(0, 0)

    def step(i, carry):
        hist(0)
        cells(2 * i + 1, 1)
        hist(1)
        cells(2 * i + 2, 0)
        written(2 * i, 2).start()
        return carry

    lax.fori_loop(0, NZ // 2 - 1, step, 0)
    hist(0)
    cells(NZ - 1, 1)
    written(NZ - 2, 2).start()
    hist(1)

    both = pltpu.matmul_pop(acc0_ref) + pltpu.matmul_pop(acc1_ref)
    lane = lax.broadcasted_iota(jnp.int32, (32, NX), 1)
    total = jnp.zeros((32, NX), jnp.float32)
    for g in range(8):
        part = both[g * 32 : (g + 1) * 32, (g // 4) * NX : (g // 4 + 1) * NX]
        total = total + jnp.where(lane // 32 == g % 4, part, 0.0)
    for shift in (64, 32):
        total = total + pltpu.roll(total, shift, 1)
    lane = lax.broadcasted_iota(jnp.int32, (16, NX), 1)
    sub = lax.broadcasted_iota(jnp.int32, (16, NX), 0)
    plain = total[0:16]
    upper = total[16:32] + pltpu.roll(plain, NX - 16, 1)

    def repeated(a):
        a = jnp.where(lane % 32 < 16, a, 0.0)
        return a + pltpu.roll(a, 16, 1)

    plain = repeated(plain)
    upper = repeated(upper)
    beside = pltpu.roll(upper, 1, 1)
    carried = jnp.where(sub == 0, 0.0, pltpu.roll(beside, 1, 0))
    counts = plain - upper + jnp.where(lane % 16 == 0, carried, beside)
    tops = [
        jnp.sum(jnp.where(sub == 8 * h + lane // 16, counts, 0.0), axis=0, keepdims=True)
        for h in range(2)
    ]
    high = jnp.max(stat_ref[1], axis=0, keepdims=True)
    low = jnp.min(stat_ref[2], axis=0, keepdims=True)
    high = jnp.maximum(high, pltpu.roll(high, NX // 2, 1))
    low = jnp.minimum(low, pltpu.roll(low, NX // 2, 1))
    extremes = jnp.where(lane[0:1] < NX // 2, high, low)
    tile = jnp.concatenate(
        tops + [jnp.sum(stat_ref[0], axis=0, keepdims=True), extremes], axis=0
    )
    red_ref[...] = jnp.broadcast_to(tile[None], red_ref.shape)
    written(0, NZ).wait()


def cells(first, beyond, x, squares, halos, peers):
    args = [in_vmem(a) for a in (x, squares, *halos)]
    _, mag, red = pl.pallas_call(
        cells_kernel,
        in_specs=[SMEM, SMEM] + [VMEM] * 4,
        out_specs=(VMEM, pl.BlockSpec(memory_space=pl.ANY), VMEM),
        out_shape=(
            vmem_out(NZ, NY, NX),
            jax.ShapeDtypeStruct((NZ, NY, NX), jnp.float32),
            vmem_out(peers, 4, NX),
        ),
        scratch_shapes=[
            pltpu.VMEM((2 * ROW, NX), jnp.float32),
            pltpu.VMEM((4, NY, NX), jnp.float32),
            pltpu.VMEM((4, NY, NX), jnp.float32),
            pltpu.VMEM((3, 8, NX), jnp.float32),
            pltpu.SemaphoreType.DMA((1,)),
        ],
        input_output_aliases={3: 0},
        name="cells",
    )(first, beyond, *args)
    return mag, red


def merged(a_ref):
    a = a_ref[...]
    lane = lax.broadcasted_iota(jnp.int32, (1, NX), 1)
    high = jnp.max(a[:, 3:4, :], axis=0)
    low = jnp.min(a[:, 3:4, :], axis=0)
    return jnp.sum(a[:, 0:3, :], axis=0), jnp.where(lane < NX // 2, high, low)


def merge_kernel(a_ref, out_ref):
    tile = jnp.concatenate(merged(a_ref), axis=0)
    out_ref[...] = jnp.broadcast_to(tile[None], out_ref.shape)


def merge(a, peers):
    return pl.pallas_call(
        merge_kernel,
        in_specs=[VMEM],
        out_specs=VMEM,
        out_shape=vmem_out(peers, 4, NX),
        name="merge",
    )(in_vmem(a))


def final_kernel(first_ref, beyond_ref, a_ref, hist_ref, stats_ref):
    summed, extremes = merged(a_ref)
    total_cells = 134217728.0
    counts = summed[0:2]
    hist_ref[...] = counts * (BINS / total_cells)
    lane = lax.broadcasted_iota(jnp.int32, (2, NX), 1)
    bins = lax.broadcasted_iota(jnp.int32, (2, NX), 0) * NX + lane
    inside = (bins >= first_ref[0]) & (bins < beyond_ref[0])
    low_half = lane[0:1] < NX // 2
    stats_ref[0] = jnp.min(jnp.where(low_half, 3.0e38, extremes))
    stats_ref[1] = jnp.max(jnp.where(low_half, extremes, -3.0e38))
    stats_ref[2] = jnp.sum(summed[2:3]) / total_cells
    stats_ref[3] = jnp.sum(jnp.where(inside, counts, 0.0)) / total_cells


def final(first, beyond, a):
    hist, stats = pl.pallas_call(
        final_kernel,
        in_specs=[SMEM, SMEM, VMEM],
        out_specs=(VMEM, SMEM),
        out_shape=(
            jax.ShapeDtypeStruct((2, NX), jnp.float32),
            jax.ShapeDtypeStruct((4,), jnp.float32),
        ),
        name="final",
    )(first, beyond, in_vmem(a))
    return hist.reshape(BINS), stats


def swapped(part, axis, side):
    count = lax.axis_size(axis)
    pairs = [((i + side) % count, (i + 1 + side) % count) for i in range(0, count, 2)]
    return lax.ppermute(part, axis, pairs + [(b, a) for a, b in pairs])


STARTS = ("x_a", "x_b", "z_a", "z_b", "y_a", "y_b")


def on_device(x, first, beyond):
    x, *sends = pack(x)
    xa, xb, ya, yb, za, zb = sends
    got = {}
    for name, part, axis in zip(STARTS, (xa, xb, za, zb, ya, yb), (GX, GX, GZ, GZ, "gy", "gy")):
        got[name] = swapped(part, axis, 0 if name[-1] == "a" else 1)
    squares = xz_squares(x, (xa, xb), [got[name] for name in STARTS[:4]])
    mag, red = cells(first, beyond, x, squares, [got[name] for name in STARTS[4:]], lax.axis_size(GX_GZ))
    red = lax.all_to_all(red, GX_GZ, 0, 0)
    red = merge(red, lax.axis_size("gy"))
    red = lax.all_to_all(red, "gy", 0, 0)
    hist, stats = final(first, beyond, red)
    return mag, hist, stats


def solution(mesh):
    finer = Mesh(
        mesh.devices.reshape(2, 2, mesh.shape["gy"], 2, 4), ("gx_0", "gx_1", "gy", "gz_0", "gz_1")
    )
    return jax.shard_map(
        on_device,
        mesh=finer,
        in_specs=(P(GZ, "gy", GX), P(), P()),
        out_specs=(P(GZ, "gy", GX), P(), P()),
        check_vma=False,
    )
```
